16 devices in a mesh: replica: 4 (over z, y), model: 4 (over x, core).
Axes of the slice: x: 2, y: 2, z: 2, core: 2. Of those that a mesh axis runs over, the one named last changes fastest.
Arguments:
- tokens: bfloat16 [512, 2304], P('replica'), parts along dimension 0
- lengths: int32 [512], P('replica'), parts along dimension 0
- k_cache: bfloat16 [512, 4, 512, 256], P('replica'), parts along dimension 0
- v_cache: bfloat16 [512, 4, 512, 256], P('replica'), parts along dimension 0
- norm_gain: bfloat16 [2304], replicated
- w_query: bfloat16 [2304, 2048], P(None, 'model')
- w_key: bfloat16 [2304, 1024], replicated
- w_value: bfloat16 [2304, 1024], replicated
- w_out: bfloat16 [2048, 2304], P('model')
- w_gate: bfloat16 [2304, 9216], P(None, 'model')
- w_up: bfloat16 [2304, 9216], P(None, 'model')
- w_down: bfloat16 [9216, 2304], P('model')
Outputs:
- output 1: bfloat16 [512, 2304], P('replica'), parts along dimension 0
- output 2: bfloat16 [512, 4, 256], P(('replica', 'model')), parts along dimension 0
- output 3: bfloat16 [512, 4, 256], P(('replica', 'model')), parts along dimension 0
There are 4 independent parts. The reference program is written for one: setup_inputs(seed, part) draws one part's arguments, and reference() takes and returns one part's arrays. A program takes and returns all parts, laid end to end along the dimension named above; an argument that names none is the same for every part.
All inputs are finite; a program needn't handle non-finite values.
Results may differ from the reference program's by a relative error of at most 0.0047526.
Values are sent between devices in bfloat16 or wider.
A program may use at most 1.25 GiB of HBM per device.

```python
import math
import jax
import jax.numpy as jnp
from jax import lax

MODEL_DIM = 2304
HEADS = 8
KV_HEADS = 4
HEAD_DIM = 256
FFN_DIM = 9216
BATCH_SIZE = 128
CONTEXT = 512

ROPE_BASE = 10000.0
NORM_EPS = 1e-6
MASK_VALUE = -1e30
KEY_SCALE = math.sqrt(math.log(CONTEXT))
LOG_CONTEXT = int(math.log2(CONTEXT))


def normal_weight(rng_key, fan_in, fan_out, gain):
    return jax.random.normal(rng_key, (fan_in, fan_out), jnp.float32) * (gain / math.sqrt(fan_in))


def setup_inputs(seed: int = 0, part: int = 0) -> dict:
    part_keys = jax.random.split(jax.random.fold_in(jax.random.key(seed), part), 8)
    shared_keys = jax.random.split(jax.random.key(seed + 1), 8)
    query_width = HEADS * HEAD_DIM
    kv_width = KV_HEADS * HEAD_DIM
    tokens = jax.random.normal(part_keys[0], (BATCH_SIZE, MODEL_DIM), jnp.float32)
    spans = jax.random.randint(part_keys[1], (BATCH_SIZE,), 0, CONTEXT - 1)
    shifts = jax.random.randint(part_keys[2], (BATCH_SIZE,), 0, LOG_CONTEXT + 1)
    lengths = 1 + jnp.right_shift(spans, shifts)
    row_ids = jnp.arange(BATCH_SIZE)
    long_row = jax.random.randint(part_keys[3], (), 0, BATCH_SIZE)
    short_row = (long_row + jax.random.randint(part_keys[4], (), 1, BATCH_SIZE)) % BATCH_SIZE
    lengths = jnp.where(row_ids == long_row, CONTEXT - 1, lengths)
    lengths = jnp.where(row_ids == short_row, 1, lengths).astype(jnp.int32)
    cache_shape = (BATCH_SIZE, KV_HEADS, CONTEXT, HEAD_DIM)
    k_cache = jax.random.normal(part_keys[5], cache_shape, jnp.float32) * KEY_SCALE
    v_cache = jax.random.normal(part_keys[6], cache_shape, jnp.float32)
    norm_gain = jax.random.uniform(shared_keys[0], (MODEL_DIM,), jnp.float32, 0.5, 1.5)
    w_query = normal_weight(shared_keys[1], MODEL_DIM, query_width, 1.0)
    w_key = normal_weight(shared_keys[2], MODEL_DIM, kv_width, KEY_SCALE)
    w_value = normal_weight(shared_keys[3], MODEL_DIM, kv_width, 1.0)
    w_out = normal_weight(shared_keys[4], query_width, MODEL_DIM, 1.0)
    w_gate = normal_weight(shared_keys[5], MODEL_DIM, FFN_DIM, 1.0)
    w_up = normal_weight(shared_keys[6], MODEL_DIM, FFN_DIM, 1.0)
    w_down = normal_weight(shared_keys[7], FFN_DIM, MODEL_DIM, 1.0)
    return {
        'tokens': tokens.astype(jnp.bfloat16),
        'lengths': lengths,
        'k_cache': k_cache.astype(jnp.bfloat16),
        'v_cache': v_cache.astype(jnp.bfloat16),
        'norm_gain': norm_gain.astype(jnp.bfloat16),
        'w_query': w_query.astype(jnp.bfloat16),
        'w_key': w_key.astype(jnp.bfloat16),
        'w_value': w_value.astype(jnp.bfloat16),
        'w_out': w_out.astype(jnp.bfloat16),
        'w_gate': w_gate.astype(jnp.bfloat16),
        'w_up': w_up.astype(jnp.bfloat16),
        'w_down': w_down.astype(jnp.bfloat16),
    }


def rms_norm(tokens, norm_gain):
    values = tokens.astype(jnp.float32)
    mean_sq = jnp.mean(values * values, axis=-1, keepdims=True)
    return (values * lax.rsqrt(mean_sq + NORM_EPS) * norm_gain.astype(jnp.float32)).astype(jnp.bfloat16)


def apply_rope(values, positions):
    half_dim = values.shape[-1] // 2
    inv_freq = jnp.exp(jnp.arange(half_dim, dtype=jnp.float32) * (-2.0 * math.log(ROPE_BASE) / values.shape[-1]))
    angles = positions.astype(jnp.float32)[:, None, None] * inv_freq[None, None, :]
    cos_part = jnp.cos(angles)
    sin_part = jnp.sin(angles)
    first_half = values[..., :half_dim]
    second_half = values[..., half_dim:]
    return jnp.concatenate([first_half * cos_part - second_half * sin_part, second_half * cos_part + first_half * sin_part], axis=-1)


def reference(tokens, lengths, k_cache, v_cache, norm_gain, w_query, w_key, w_value, w_out, w_gate, w_up, w_down):
    group_size = HEADS // KV_HEADS
    scale = HEAD_DIM ** -0.5
    normed = rms_norm(tokens, norm_gain)
    queries = apply_rope(jnp.dot(normed, w_query, preferred_element_type=jnp.float32).reshape(BATCH_SIZE, HEADS, HEAD_DIM), lengths).astype(jnp.bfloat16)
    new_keys = apply_rope(jnp.dot(normed, w_key, preferred_element_type=jnp.float32).reshape(BATCH_SIZE, KV_HEADS, HEAD_DIM), lengths).astype(jnp.bfloat16)
    new_values = jnp.dot(normed, w_value, preferred_element_type=jnp.float32).reshape(BATCH_SIZE, KV_HEADS, HEAD_DIM).astype(jnp.bfloat16)
    positions = jnp.arange(CONTEXT)

    def one_sequence(items):
        query_row, key_rows, value_rows, key_new, value_new, length = items
        grouped = query_row.reshape(KV_HEADS, group_size, HEAD_DIM).astype(jnp.float32)
        scores = jnp.einsum('grd,gtd->grt', grouped, key_rows.astype(jnp.float32)) * scale
        scores = jnp.where(positions[None, None, :] < length, scores, MASK_VALUE)
        score_new = jnp.einsum('grd,gd->gr', grouped, key_new.astype(jnp.float32)) * scale
        peak = jnp.maximum(jnp.max(scores, axis=-1), score_new)
        weights = jnp.exp(scores - peak[:, :, None])
        weight_new = jnp.exp(score_new - peak)
        total = jnp.sum(weights, axis=-1) + weight_new
        mixed = jnp.einsum('grt,gtd->grd', weights.astype(jnp.bfloat16).astype(jnp.float32), value_rows.astype(jnp.float32))
        mixed = mixed + weight_new.astype(jnp.bfloat16).astype(jnp.float32)[:, :, None] * value_new.astype(jnp.float32)[:, None, :]
        return (mixed / total[:, :, None]).astype(jnp.bfloat16).reshape(HEADS * HEAD_DIM)

    attended = lax.map(one_sequence, (queries, k_cache, v_cache, new_keys, new_values, lengths))
    gate_act = jnp.dot(normed, w_gate, preferred_element_type=jnp.float32)
    up_act = jnp.dot(normed, w_up, preferred_element_type=jnp.float32)
    hidden = (jax.nn.silu(gate_act) * up_act).astype(jnp.bfloat16)
    summed = tokens.astype(jnp.float32) + jnp.dot(attended, w_out, preferred_element_type=jnp.float32) + jnp.dot(hidden, w_down, preferred_element_type=jnp.float32)
    return summed.astype(jnp.bfloat16), new_keys, new_values
```

```python
import functools
import math
import jax
import jax.numpy as jnp
from jax import lax
from jax.experimental import pallas as pl
from jax.experimental.pallas import tpu as pltpu
from jax.sharding import PartitionSpec as P

ROPE_BASE = 10000.0
NORM_EPS = 1e-6
MASK_VALUE = -1e30
F32 = jnp.float32
BF16 = jnp.bfloat16

FIRST = 32
GROUP = 8
CHUNK = 128
UNROLL = 8
SLOTS = 12
COLS = 256
PIECE = 384


def iota(shape, dim):
    return lax.broadcasted_iota(jnp.int32, shape, dim)


def nt_dot(a, b):
    return lax.dot_general(a, b, (((1,), (1,)), ((), ())), preferred_element_type=F32)


def nn_dot(a, b):
    return jnp.dot(a, b, preferred_element_type=F32)


def interleave(first, second):
    pieces = []
    for r in range(0, first.shape[0], GROUP):
        pieces += [first[r:r + GROUP], second[r:r + GROUP]]
    return jnp.concatenate(pieces, axis=0)


def local_kernel(dims, len_hbm, x_hbm, gain_hbm, k_hbm, v_hbm, wq_hbm, wk_hbm, wv_hbm, wg_hbm, wu_hbm,
                 u_ref, o_ref, kv_ref,
                 len_s, len_v, x_v, gain_v, wq_v, wk_v, wv_v, wg_v, wu_v, kfirst, vfirst, kbuf, vbuf, h_v,
                 tile_s, q_rows, len_rows, s_first, s_buf, snew_v, vnew_v, m_v, l_v, acc_v,
                 sems, wsems, fsems, ksems, vsems):
    batch, model_dim, head_dim, context = dims
    half = head_dim // 2
    rows = 2 * GROUP
    groups = batch // GROUP
    me = lax.axis_index('model')
    n_pieces = wg_v.shape[0]
    last_start = context - CHUNK

    def piece_copy(hbm, buf, n, which):
        return pltpu.make_async_copy(hbm.at[:, pl.ds(n * COLS, COLS)], buf.at[n], wsems.at[which, n])

    def first_copy(hbm, buf, which, n):
        seqs = pl.ds(n * (batch // 2), batch // 2)
        return pltpu.make_async_copy(hbm.at[seqs, me, pl.ds(0, FIRST), :], buf.at[seqs], fsems.at[which, n])

    head_col = pl.multiple_of(me * head_dim, 128)
    small = [
        pltpu.make_async_copy(len_hbm, len_s, sems.at[0]),
        pltpu.make_async_copy(x_hbm, x_v, sems.at[1]),
        pltpu.make_async_copy(gain_hbm, gain_v, sems.at[2]),
        pltpu.make_async_copy(len_hbm, len_v, sems.at[6]),
        pltpu.make_async_copy(wq_hbm, wq_v, sems.at[3]),
        pltpu.make_async_copy(wk_hbm.at[:, pl.ds(head_col, head_dim)], wk_v, sems.at[4]),
        pltpu.make_async_copy(wv_hbm.at[:, pl.ds(head_col, head_dim)], wv_v, sems.at[5]),
    ]
    for copy in small:
        copy.start()
    for n in range(2):
        first_copy(k_hbm, kfirst, 0, n).start()
    for n in range(2):
        first_copy(v_hbm, vfirst, 1, n).start()
    for n in range(n_pieces):
        piece_copy(wg_hbm, wg_v, n, 0).start(priority=1)
        piece_copy(wu_hbm, wu_v, n, 1).start(priority=1)

    small[0].wait()

    def fill(r, t):
        for i in range(GROUP):
            b = r * GROUP + i
            for c in range((context - FIRST + CHUNK - 1) // CHUNK):
                tile_s[t + c] = b * 8 + c
            t = t + lax.shift_right_logical(len_s[0, b] + (CHUNK - 1 - FIRST), CHUNK.bit_length() - 1)
        return t
    tiles = lax.fori_loop(0, groups, fill, 0)
    for j in range(UNROLL):
        tile_s[tiles + j] = 7
    bodies = (tiles + UNROLL - 1) // UNROLL

    def issue(hbm, buf, bsems, body):
        slot = lax.rem(body, SLOTS)
        for j in range(UNROLL):
            code = tile_s[body * UNROLL + j]
            start = jnp.minimum(FIRST + (code & 7) * CHUNK, last_start)
            pltpu.make_async_copy(hbm.at[lax.shift_right_logical(code, 3), me, pl.ds(pl.multiple_of(start, FIRST), CHUNK), :],
                                  buf.at[slot, j], bsems.at[slot]).start()

    def issue_both(body, _):
        issue(k_hbm, kbuf, ksems, body)
        issue(v_hbm, vbuf, vsems, body)
        return 0

    def wait_body(buf, bsems, body):
        slot = lax.rem(body, SLOTS)
        pltpu.make_async_copy(buf.at[slot], buf.at[slot], bsems.at[slot]).wait()

    lax.fori_loop(0, jnp.minimum(bodies, SLOTS), issue_both, 0)

    small[3].wait()
    ii, jj = iota((batch, batch), 0), iota((batch, batch), 1)
    len_col = jnp.sum(jnp.where(ii == jj, len_v[...].astype(F32), 0.0), axis=1, keepdims=True)
    len_wide = jnp.broadcast_to(len_col, (batch, 128))
    len_rows[...] = interleave(len_wide, len_wide)
    freq = jnp.exp(iota((1, half), 1).astype(F32) * (-2.0 * math.log(ROPE_BASE) / head_dim))
    angles = len_col * freq
    cos_part, sin_part = jnp.cos(angles), jnp.sin(angles)

    def rope(v):
        a, b = v[:, :half], v[:, half:]
        return jnp.concatenate([a * cos_part - b * sin_part, b * cos_part + a * sin_part], axis=1).astype(BF16)

    small[1].wait()
    small[2].wait()
    x = x_v[...].astype(F32)
    mean_sq = jnp.mean(x * x, axis=-1, keepdims=True)
    h_v[...] = (x * lax.rsqrt(mean_sq + NORM_EPS) * gain_v[...].astype(F32).reshape(1, model_dim)).astype(BF16)

    small[4].wait()
    small[5].wait()
    small[6].wait()
    h = h_v[...]
    q = nn_dot(h, wq_v[...])
    k_new = rope(nn_dot(h, wk_v[...]))
    v_new = nn_dot(h, wv_v[...]).astype(BF16)
    kv_ref[:, :head_dim] = k_new
    kv_ref[:, head_dim:] = v_new
    vnew_v[...] = v_new.astype(F32)
    scale = head_dim ** -0.5
    q_heads = [rope(q[:, n * head_dim:(n + 1) * head_dim]).astype(F32) for n in range(2)]
    q_rows[...] = interleave(*q_heads).astype(BF16)
    k_wide = k_new.astype(F32)
    s_new = [jnp.broadcast_to(jnp.sum(qh * k_wide, axis=1, keepdims=True) * scale, (batch, 128)) for qh in q_heads]
    snew_v[...] = interleave(*s_new)

    lane, sub = iota((rows, GROUP * FIRST), 1), iota((rows, GROUP * FIRST), 0)
    own_lane = lax.shift_right_logical(lane, FIRST.bit_length() - 1) == (sub & (GROUP - 1))
    token = (lane & (FIRST - 1)).astype(F32)
    for n in range(2):
        first_copy(k_hbm, kfirst, 0, n).wait()
    for g in range(groups):
        keys = kfirst[g * GROUP:(g + 1) * GROUP].reshape(GROUP * FIRST, head_dim)
        s = nt_dot(q_rows[g * rows:(g + 1) * rows, :], keys)
        reach = len_rows[g * rows:(g + 1) * rows, :]
        s = jnp.where(own_lane & (token < jnp.concatenate([reach, reach], axis=1)), s * scale, MASK_VALUE)
        s_first[g] = s
        m_v[g * rows:(g + 1) * rows, :] = jnp.maximum(snew_v[g * rows:(g + 1) * rows, :], jnp.maximum(s[:, :128], s[:, 128:]))

    lane, sub = iota((rows, CHUNK), 1), iota((rows, CHUNK), 0) & (GROUP - 1)

    def tile_of(t):
        code = tile_s[t]
        b = lax.shift_right_logical(code, 3)
        row = pl.multiple_of(lax.shift_right_logical(b, GROUP.bit_length() - 1) * rows, rows)
        return b & (GROUP - 1), row, FIRST + (code & 7) * CHUNK

    def score_body(body, _):
        wait_body(kbuf, ksems, body)
        slot = lax.rem(body, SLOTS)
        scores = []
        for j in range(UNROLL):
            i, row, begin = tile_of(body * UNROLL + j)
            s = nt_dot(q_rows[pl.ds(row, rows), :], kbuf[slot, j])
            position = lane + jnp.minimum(begin, last_start)
            valid = (sub == i) & (position >= begin) & (position.astype(F32) < len_rows[pl.ds(row, rows), :])
            scores.append((row, jnp.where(valid, s * scale, MASK_VALUE)))
        for j, (row, s) in enumerate(scores):
            s_buf[body * UNROLL + j] = s
            m_v[pl.ds(row, rows), :] = jnp.maximum(m_v[pl.ds(row, rows), :], s)

        @pl.when(body + SLOTS < bodies)
        def _():
            issue(k_hbm, kbuf, ksems, body + SLOTS)
        return 0
    lax.fori_loop(0, bodies, score_body, 0)

    peak = jnp.max(m_v[...], axis=1, keepdims=True)
    m_v[...] = jnp.broadcast_to(peak, m_v.shape)

    for n in range(2):
        first_copy(v_hbm, vfirst, 1, n).wait()
    for g in range(groups):
        m = m_v[g * rows:(g + 1) * rows, :]
        p = jnp.exp(s_first[g] - jnp.concatenate([m, m], axis=1))
        l_v[g * rows:(g + 1) * rows, :] = p[:, :128] + p[:, 128:]
        acc_v[g * rows:(g + 1) * rows, :] = nn_dot(p.astype(BF16), vfirst[g * GROUP:(g + 1) * GROUP].reshape(GROUP * FIRST, head_dim))

    def value_body(body, _):
        wait_body(vbuf, vsems, body)
        slot = lax.rem(body, SLOTS)
        mixed = []
        for j in range(UNROLL):
            _, row, _ = tile_of(body * UNROLL + j)
            p = jnp.exp(s_buf[body * UNROLL + j] - m_v[pl.ds(row, rows), :])
            mixed.append((row, p, nn_dot(p.astype(BF16), vbuf[slot, j])))
        for row, p, o in mixed:
            l_v[pl.ds(row, rows), :] += p
            acc_v[pl.ds(row, rows), :] += o

        @pl.when(body + SLOTS < bodies)
        def _():
            issue(v_hbm, vbuf, vsems, body + SLOTS)
        return 0
    lax.fori_loop(0, bodies, value_body, 0)

    e_new = jnp.exp(snew_v[...] - m_v[...])
    total = jnp.sum(l_v[...], axis=1, keepdims=True) + e_new[:, :1]
    weight_new = e_new[:, :1].astype(BF16).astype(F32)
    mixed = (acc_v[...] + weight_new * interleave(vnew_v[...], vnew_v[...])) / total
    for head in range(2):
        o_head = jnp.concatenate([mixed[g * rows + head * GROUP:g * rows + (head + 1) * GROUP] for g in range(groups)], axis=0)
        o_ref[:, head * head_dim:(head + 1) * head_dim] = o_head.astype(BF16)

    for n in range(n_pieces):
        piece_copy(wg_hbm, wg_v, n, 0).wait()
        piece_copy(wu_hbm, wu_v, n, 1).wait()
        gate = nn_dot(h_v[...], wg_v[n])
        up = nn_dot(h_v[...], wu_v[n])
        u_ref[:, n * COLS:(n + 1) * COLS] = (gate * jax.nn.sigmoid(gate) * up).astype(BF16)


def reduce_kernel(dims, x_hbm, u_v, o_v, kv_v, wo_hbm, wd_hbm,
                  y_v, kn_ref, vn_ref,
                  x_v, kv_all, kv_rows, wo_v, wd_v, part, from_sib, half_sum, from_chip,
                  sems, wsems, kv_send, kv_recv, rs_send, rs_recv, xs_send, xs_recv, gx_send, gx_recv, gs_send, gs_recv, gf_send, gf_recv):
    batch, head_dim = dims
    quarter = batch // 4
    pieces = part.shape[0]
    me = lax.axis_index('model')
    chip, core = me // 2, me % 2
    sibling = chip * 2 + (1 - core)
    across = (1 - chip) * 2 + core

    def rows_of(chip_, core_):
        return pl.multiple_of(core_ * (2 * quarter) + chip_ * quarter, quarter)

    own = rows_of(chip, core)
    own_half = pl.multiple_of(core * (2 * quarter), 2 * quarter)
    sib_half = pl.multiple_of((1 - core) * (2 * quarter), 2 * quarter)

    def weight_copies(n):
        cols = pl.ds(n * PIECE, PIECE)
        return (pltpu.make_async_copy(wo_hbm.at[:, cols], wo_v.at[:, cols], wsems.at[0, n]),
                pltpu.make_async_copy(wd_hbm.at[:, cols], wd_v.at[:, cols], wsems.at[1, n]))

    x_copy = pltpu.make_async_copy(x_hbm.at[pl.ds(own, quarter), :], x_v, sems.at[0])
    for n in range(pieces):
        for copy in weight_copies(n):
            copy.start()
    x_copy.start()

    barrier = pltpu.get_barrier_semaphore()
    for d in range(1, 4):
        pl.semaphore_signal(barrier, inc=1, device_id={'model': (me + d) % 4}, device_id_type=pl.DeviceIdType.MESH)
    pl.semaphore_wait(barrier, 3)

    kv_sends = []
    for d in range(1, 4):
        to = (me + d) % 4
        kv_sends.append(pltpu.make_async_remote_copy(
            src_ref=kv_v.at[pl.ds(pl.multiple_of(to * quarter, quarter), quarter), :], dst_ref=kv_all.at[me],
            send_sem=kv_send.at[d - 1], recv_sem=kv_recv.at[d - 1], device_id={'model': to}, device_id_type=pl.DeviceIdType.MESH))
    for copy in kv_sends:
        copy.start()
    kv_all[me] = kv_v[pl.ds(pl.multiple_of(me * quarter, quarter), quarter), :]

    def remote(src, dst, send, recv, n, to):
        return pltpu.make_async_remote_copy(src_ref=src, dst_ref=dst, send_sem=send.at[n], recv_sem=recv.at[n],
                                            device_id={'model': to}, device_id_type=pl.DeviceIdType.MESH)

    def rs(n):
        return remote(part.at[n, pl.ds(sib_half, 2 * quarter), :], from_sib.at[n], rs_send, rs_recv, n, sibling)

    def xs(n):
        return remote(half_sum.at[n, pl.ds(pl.multiple_of((1 - chip) * quarter, quarter), quarter), :], from_chip.at[n], xs_send, xs_recv, n, across)

    def y_piece(row, n):
        return y_v.at[pl.ds(row, quarter), pl.ds(n * PIECE, PIECE)]

    def gx(n):
        return remote(y_piece(own, n), y_piece(own, n), gx_send, gx_recv, n, across)

    def gs(n):
        return remote(y_piece(own, n), y_piece(own, n), gs_send, gs_recv, n, sibling)

    def gf(n):
        other = rows_of(1 - chip, core)
        return remote(y_piece(other, n), y_piece(other, n), gf_send, gf_recv, n, sibling)

    def sum_chip(n):
        rs(n).wait_recv()
        half_sum[n] = part[n, pl.ds(own_half, 2 * quarter), :] + from_sib[n]
        xs(n).start()

    def finish(n):
        xs(n).wait_recv()
        cols = slice(n * PIECE, (n + 1) * PIECE)
        mine = half_sum[n, pl.ds(pl.multiple_of(chip * quarter, quarter), quarter), :] + from_chip[n]
        y_v[pl.ds(own, quarter), cols] = (x_v[:, cols].astype(F32) + mine).astype(BF16)
        gx(n).start()
        gs(n).start()

    def forward(n):
        gx(n).wait_recv()
        gf(n).start()

    for n in range(pieces):
        for copy in weight_copies(n):
            copy.wait()
        cols = slice(n * PIECE, (n + 1) * PIECE)
        part[n] = nn_dot(o_v[...], wo_v[:, cols]) + nn_dot(u_v[...], wd_v[:, cols])
        rs(n).start()
        if n >= 1:
            sum_chip(n - 1)
    sum_chip(pieces - 1)

    for copy in kv_sends:
        copy.wait_recv()
    for h in range(4):
        kv_rows[0, :, h, :] = kv_all[h, :, :head_dim].astype(F32)
        kv_rows[1, :, h, :] = kv_all[h, :, head_dim:].astype(F32)
    kn_ref[...] = kv_rows[0].astype(BF16)
    vn_ref[...] = kv_rows[1].astype(BF16)

    x_copy.wait()
    for n in range(pieces):
        finish(n)
    for n in range(pieces):
        forward(n)
    for n in range(pieces):
        gs(n).wait_recv()
        gf(n).wait_recv()

    for copy in kv_sends:
        copy.wait_send()
    for n in range(pieces):
        for copy in (rs(n), xs(n), gx(n), gs(n), gf(n)):
            copy.wait_send()


def solution(mesh):
    def local_step(tokens, lengths, k_cache, v_cache, norm_gain, w_query, w_key, w_value, w_out, w_gate, w_up, w_down):
        batch, model_dim = tokens.shape
        kv_heads, context, head_dim = k_cache.shape[1:]
        ffn = w_gate.shape[1]
        q_width = w_query.shape[1]
        rows = 2 * batch
        max_tiles = batch * (context // CHUNK) + UNROLL
        any_spec = pl.BlockSpec(memory_space=pl.ANY)
        vmem_spec = pl.BlockSpec(memory_space=pltpu.VMEM)
        dma = pltpu.SemaphoreType.DMA

        pieces = ffn // COLS
        hidden, attended, kv_new = pl.pallas_call(
            functools.partial(local_kernel, (batch, model_dim, head_dim, context)),
            name='attend_and_gate',
            out_shape=[pltpu.VMEM((batch, ffn), BF16), pltpu.VMEM((batch, q_width), BF16), pltpu.VMEM((batch, 2 * head_dim), BF16)],
            in_specs=[any_spec] * 10,
            out_specs=[vmem_spec] * 3,
            scratch_shapes=[
                pltpu.SMEM((1, batch), jnp.int32),
                pltpu.VMEM((1, batch), jnp.int32),
                pltpu.VMEM((batch, model_dim), BF16),
                pltpu.VMEM((model_dim,), BF16),
                pltpu.VMEM((model_dim, q_width), BF16),
                pltpu.VMEM((model_dim, head_dim), BF16),
                pltpu.VMEM((model_dim, head_dim), BF16),
                pltpu.VMEM((pieces, model_dim, COLS), BF16),
                pltpu.VMEM((pieces, model_dim, COLS), BF16),
                pltpu.VMEM((batch, FIRST, head_dim), BF16),
                pltpu.VMEM((batch, FIRST, head_dim), BF16),
                pltpu.VMEM((SLOTS, UNROLL, CHUNK, head_dim), BF16),
                pltpu.VMEM((SLOTS, UNROLL, CHUNK, head_dim), BF16),
                pltpu.VMEM((batch, model_dim), BF16),
                pltpu.SMEM((max_tiles,), jnp.int32),
                pltpu.VMEM((rows, head_dim), BF16),
                pltpu.VMEM((rows, 128), F32),
                pltpu.VMEM((batch // GROUP, 2 * GROUP, GROUP * FIRST), F32),
                pltpu.VMEM((max_tiles, 2 * GROUP, CHUNK), F32),
                pltpu.VMEM((rows, 128), F32),
                pltpu.VMEM((batch, head_dim), F32),
                pltpu.VMEM((rows, 128), F32),
                pltpu.VMEM((rows, 128), F32),
                pltpu.VMEM((rows, head_dim), F32),
                dma((7,)),
                dma((2, pieces)),
                dma((2, 2)),
                dma((SLOTS,)),
                dma((SLOTS,)),
            ],
            compiler_params=pltpu.CompilerParams(has_side_effects=True, vmem_limit_bytes=54 << 20),
        )(lengths.reshape(1, batch), tokens, norm_gain, k_cache, v_cache, w_query, w_key, w_value, w_gate, w_up)

        quarter = batch // 4
        pieces = model_dim // PIECE
        new_shape = (quarter, kv_heads, head_dim)
        out_shapes = [(batch, model_dim), new_shape, new_shape]
        return pl.pallas_call(
            functools.partial(reduce_kernel, (batch, head_dim)),
            name='project_and_sum',
            out_shape=[pltpu.VMEM(shape, BF16) for shape in out_shapes],
            in_specs=[any_spec, vmem_spec, vmem_spec, vmem_spec, any_spec, any_spec],
            out_specs=[vmem_spec] * 3,
            scratch_shapes=[
                pltpu.VMEM((quarter, model_dim), BF16),
                pltpu.VMEM((4, quarter, 2 * head_dim), BF16),
                pltpu.VMEM((2, quarter, 4, head_dim), F32),
                pltpu.VMEM((q_width, model_dim), BF16),
                pltpu.VMEM((ffn, model_dim), BF16),
                pltpu.VMEM((pieces, batch, PIECE), F32),
                pltpu.VMEM((pieces, 2 * quarter, PIECE), F32),
                pltpu.VMEM((pieces, 2 * quarter, PIECE), F32),
                pltpu.VMEM((pieces, quarter, PIECE), F32),
                dma((1,)),
                dma((2, pieces)),
                dma((3,)), dma((3,)),
            ] + [dma((pieces,))] * 10,
            compiler_params=pltpu.CompilerParams(collective_id=0, has_side_effects=True, vmem_limit_bytes=48 << 20),
        )(tokens, hidden, attended, kv_new, w_out, w_down)

    in_specs = (P('replica', None), P('replica'), P('replica', None, None, None), P('replica', None, None, None), P(None), P(None, 'model'), P(None, None), P(None, None), P('model', None), P(None, 'model'), P(None, 'model'), P('model', None))
    out_specs = (P('replica', None), P(('replica', 'model'), None, None), P(('replica', 'model'), None, None))
    return jax.shard_map(local_step, mesh=mesh, in_specs=in_specs, out_specs=out_specs, check_vma=False)
```

```python
import functools
import math
import jax
import jax.numpy as jnp
from jax import lax
from jax.experimental import pallas as pl
from jax.experimental.pallas import tpu as pltpu
from jax.sharding import PartitionSpec as P

ROPE_BASE = 10000.0
NORM_EPS = 1e-6
MASK_VALUE = -1e30
F32 = jnp.float32
BF16 = jnp.bfloat16

FIRST = 32
GROUP = 8
CHUNK = 128
UNROLL = 16
SLOTS = 6
COLS = 256
WIDTHS = (256, 256, 512, 512, 512, 256)


def iota(shape, dim):
    return lax.broadcasted_iota(jnp.int32, shape, dim)


def nt_dot(a, b):
    return lax.dot_general(a, b, (((1,), (1,)), ((), ())), preferred_element_type=F32)


def nn_dot(a, b):
    return jnp.dot(a, b, preferred_element_type=F32)


def interleave(first, second):
    pieces = []
    for r in range(0, first.shape[0], GROUP):
        pieces += [first[r:r + GROUP], second[r:r + GROUP]]
    return jnp.concatenate(pieces, axis=0)


def local_kernel(dims, len_hbm, x_hbm, gain_hbm, k_hbm, v_hbm, wq_hbm, wk_hbm, wv_hbm, wg_hbm, wu_hbm,
                 u_ref, o_ref, kv_ref,
                 len_s, len_v, x_v, gain_v, wq_v, wk_v, wv_v, wg_v, wu_v, kfirst, vfirst, kbuf, vbuf, h_v,
                 tile_s, size_s, q_rows, len_rows, s_first, s_buf, snew_v, vnew_v, m_v, l_v, acc_v,
                 sems, wsems, fsems, ksems, vsems):
    batch, model_dim, head_dim, context = dims
    half = head_dim // 2
    rows = 2 * GROUP
    groups = batch // GROUP
    me = lax.axis_index('model')
    n_pieces = wg_v.shape[0]
    blocks = CHUNK // FIRST

    def piece_copy(hbm, buf, n, which):
        return pltpu.make_async_copy(hbm.at[:, pl.ds(n * COLS, COLS)], buf.at[n], wsems.at[which, n])

    def first_copy(hbm, buf, which, n):
        seqs = pl.ds(n * (batch // 2), batch // 2)
        return pltpu.make_async_copy(hbm.at[seqs, me, 0], buf.at[seqs], fsems.at[which, n])

    head_col = pl.multiple_of(me * head_dim, 128)
    small = [
        pltpu.make_async_copy(len_hbm, len_s, sems.at[0]),
        pltpu.make_async_copy(x_hbm, x_v, sems.at[1]),
        pltpu.make_async_copy(gain_hbm, gain_v, sems.at[2]),
        pltpu.make_async_copy(len_hbm, len_v, sems.at[6]),
        pltpu.make_async_copy(wq_hbm, wq_v, sems.at[3]),
        pltpu.make_async_copy(wk_hbm.at[:, pl.ds(head_col, head_dim)], wk_v, sems.at[4]),
        pltpu.make_async_copy(wv_hbm.at[:, pl.ds(head_col, head_dim)], wv_v, sems.at[5]),
    ]
    for copy in small:
        copy.start()
    for n in range(2):
        first_copy(k_hbm, kfirst, 0, n).start()
    for n in range(2):
        first_copy(v_hbm, vfirst, 1, n).start()
    for n in range(n_pieces):
        piece_copy(wg_hbm, wg_v, n, 0).start(priority=1)
        piece_copy(wu_hbm, wu_v, n, 1).start(priority=1)

    vbuf[...] = jnp.zeros_like(vbuf)
    small[0].wait()

    def fill(r, t):
        for i in range(GROUP):
            b = r * GROUP + i
            for c in range((context - FIRST + CHUNK - 1) // CHUNK):
                tile_s[t + c] = b * 8 + c
            t = t + lax.shift_right_logical(len_s[0, b] + (CHUNK - 1 - FIRST), CHUNK.bit_length() - 1)
        return t
    tiles = lax.fori_loop(0, groups, fill, 0)
    for j in range(UNROLL):
        tile_s[tiles + j] = 7
    bodies = (tiles + UNROLL - 1) // UNROLL

    def issue(hbm, buf, bsems, body):
        slot = lax.rem(body, SLOTS)
        total = 0
        for j in range(UNROLL):
            code = tile_s[body * UNROLL + j]
            b = lax.shift_right_logical(code, 3)
            start = jnp.minimum(1 + (code & 7) * blocks, context // FIRST - 1)
            end = lax.shift_right_logical(len_s[0, b] + (FIRST - 1), FIRST.bit_length() - 1)
            count = jnp.clip(end - start, 1, blocks)
            pltpu.make_async_copy(hbm.at[b, me, pl.ds(start, count)], buf.at[slot, pl.ds(j * blocks, count)], bsems.at[slot]).start()
            total += count
        size_s[body] = total

    def issue_both(body, _):
        issue(k_hbm, kbuf, ksems, body)
        issue(v_hbm, vbuf, vsems, body)
        return 0

    def wait_body(buf, bsems, body):
        slot = lax.rem(body, SLOTS)
        filled = buf.at[slot, pl.ds(0, size_s[body])]
        pltpu.make_async_copy(filled, filled, bsems.at[slot]).wait()

    lax.fori_loop(0, jnp.minimum(bodies, SLOTS), issue_both, 0)

    small[3].wait()
    ii, jj = iota((batch, batch), 0), iota((batch, batch), 1)
    len_col = jnp.sum(jnp.where(ii == jj, len_v[...].astype(F32), 0.0), axis=1, keepdims=True)
    len_wide = jnp.broadcast_to(len_col, (batch, 128))
    len_rows[...] = interleave(len_wide, len_wide)
    freq = jnp.exp(iota((1, half), 1).astype(F32) * (-2.0 * math.log(ROPE_BASE) / head_dim))
    angles = len_col * freq
    cos_part, sin_part = jnp.cos(angles), jnp.sin(angles)

    def rope(v):
        a, b = v[:, :half], v[:, half:]
        return jnp.concatenate([a * cos_part - b * sin_part, b * cos_part + a * sin_part], axis=1).astype(BF16)

    small[1].wait()
    small[2].wait()
    x = x_v[...].astype(F32)
    mean_sq = jnp.mean(x * x, axis=-1, keepdims=True)
    h_v[...] = (x * lax.rsqrt(mean_sq + NORM_EPS) * gain_v[...].astype(F32).reshape(1, model_dim)).astype(BF16)

    small[4].wait()
    small[5].wait()
    small[6].wait()
    h = h_v[...]
    q = nn_dot(h, wq_v[...])
    k_new = rope(nn_dot(h, wk_v[...]))
    v_new = nn_dot(h, wv_v[...]).astype(BF16)
    kv_ref[:, :head_dim] = k_new
    kv_ref[:, head_dim:] = v_new
    vnew_v[...] = v_new.astype(F32)
    scale = head_dim ** -0.5
    q_heads = [rope(q[:, n * head_dim:(n + 1) * head_dim]).astype(F32) for n in range(2)]
    q_rows[...] = interleave(*q_heads).astype(BF16)
    k_wide = k_new.astype(F32)
    s_new = [jnp.broadcast_to(jnp.sum(qh * k_wide, axis=1, keepdims=True) * scale, (batch, 128)) for qh in q_heads]
    snew_v[...] = interleave(*s_new)

    lane, sub = iota((rows, GROUP * FIRST), 1), iota((rows, GROUP * FIRST), 0)
    own_lane = lax.shift_right_logical(lane, FIRST.bit_length() - 1) == (sub & (GROUP - 1))
    token = (lane & (FIRST - 1)).astype(F32)
    for n in range(2):
        first_copy(k_hbm, kfirst, 0, n).wait()
    for g in range(groups):
        keys = kfirst[g * GROUP:(g + 1) * GROUP].reshape(GROUP * FIRST, head_dim)
        s = nt_dot(q_rows[g * rows:(g + 1) * rows, :], keys)
        reach = len_rows[g * rows:(g + 1) * rows, :]
        s = jnp.where(own_lane & (token < jnp.concatenate([reach, reach], axis=1)), s * scale, MASK_VALUE)
        s_first[g] = s
        m_v[g * rows:(g + 1) * rows, :] = jnp.maximum(snew_v[g * rows:(g + 1) * rows, :], jnp.maximum(s[:, :128], s[:, 128:]))

    lane, sub = iota((rows, CHUNK), 1), iota((rows, CHUNK), 0) & (GROUP - 1)

    def tile_of(t):
        code = tile_s[t]
        b = lax.shift_right_logical(code, 3)
        row = pl.multiple_of(lax.shift_right_logical(b, GROUP.bit_length() - 1) * rows, rows)
        return b & (GROUP - 1), row, FIRST + (code & 7) * CHUNK

    def score_body(body, _):
        wait_body(kbuf, ksems, body)
        slot = lax.rem(body, SLOTS)
        scores = []
        for j in range(UNROLL):
            i, row, begin = tile_of(body * UNROLL + j)
            s = nt_dot(q_rows[pl.ds(row, rows), :], kbuf[slot, j * blocks:(j + 1) * blocks].reshape(CHUNK, head_dim))
            valid = (sub == i) & ((lane + begin).astype(F32) < len_rows[pl.ds(row, rows), :])
            scores.append((row, jnp.where(valid, s * scale, MASK_VALUE)))
        for j, (row, s) in enumerate(scores):
            s_buf[body * UNROLL + j] = s
            m_v[pl.ds(row, rows), :] = jnp.maximum(m_v[pl.ds(row, rows), :], s)

        @pl.when(body + SLOTS < bodies)
        def _():
            issue(k_hbm, kbuf, ksems, body + SLOTS)
        return 0
    lax.fori_loop(0, bodies, score_body, 0)

    peak = jnp.max(m_v[...], axis=1, keepdims=True)
    m_v[...] = jnp.broadcast_to(peak, m_v.shape)

    for n in range(2):
        first_copy(v_hbm, vfirst, 1, n).wait()
    for g in range(groups):
        m = m_v[g * rows:(g + 1) * rows, :]
        p = jnp.exp(s_first[g] - jnp.concatenate([m, m], axis=1))
        l_v[g * rows:(g + 1) * rows, :] = p[:, :128] + p[:, 128:]
        acc_v[g * rows:(g + 1) * rows, :] = nn_dot(p.astype(BF16), vfirst[g * GROUP:(g + 1) * GROUP].reshape(GROUP * FIRST, head_dim))

    def value_body(body, _):
        wait_body(vbuf, vsems, body)
        slot = lax.rem(body, SLOTS)
        mixed = []
        for j in range(UNROLL):
            _, row, _ = tile_of(body * UNROLL + j)
            p = jnp.exp(s_buf[body * UNROLL + j] - m_v[pl.ds(row, rows), :])
            mixed.append((row, p, nn_dot(p.astype(BF16), vbuf[slot, j * blocks:(j + 1) * blocks].reshape(CHUNK, head_dim))))
        for row, p, o in mixed:
            l_v[pl.ds(row, rows), :] += p
            acc_v[pl.ds(row, rows), :] += o

        @pl.when(body + SLOTS < bodies)
        def _():
            issue(v_hbm, vbuf, vsems, body + SLOTS)
        return 0
    lax.fori_loop(0, bodies, value_body, 0)

    e_new = jnp.exp(snew_v[...] - m_v[...])
    total = jnp.sum(l_v[...], axis=1, keepdims=True) + e_new[:, :1]
    weight_new = e_new[:, :1].astype(BF16).astype(F32)
    mixed = (acc_v[...] + weight_new * interleave(vnew_v[...], vnew_v[...])) / total
    for head in range(2):
        o_head = jnp.concatenate([mixed[g * rows + head * GROUP:g * rows + (head + 1) * GROUP] for g in range(groups)], axis=0)
        o_ref[:, head * head_dim:(head + 1) * head_dim] = o_head.astype(BF16)

    for n in range(n_pieces):
        piece_copy(wg_hbm, wg_v, n, 0).wait()
        piece_copy(wu_hbm, wu_v, n, 1).wait()
        gate = nn_dot(h_v[...], wg_v[n])
        up = nn_dot(h_v[...], wu_v[n])
        u_ref[:, n * COLS:(n + 1) * COLS] = (gate * jax.nn.sigmoid(gate) * up).astype(BF16)


def reduce_kernel(dims, x_hbm, u_v, o_v, kv_v, wo_hbm, wd_hbm,
                  y_v, kn_ref, vn_ref,
                  x_v, kv_all, kv_rows, wo_v, wd_v, part, from_sib, half_sum, from_chip,
                  sems, wsems, kv_send, kv_recv, rs_send, rs_recv, xs_send, xs_recv, gx_send, gx_recv, gs_send, gs_recv, gf_send, gf_recv):
    batch, head_dim = dims
    quarter = batch // 4
    pieces = len(WIDTHS)

    def cols_of(n):
        return pl.ds(sum(WIDTHS[:n]), WIDTHS[n])

    me = lax.axis_index('model')
    chip, core = me // 2, me % 2
    sibling = chip * 2 + (1 - core)
    across = (1 - chip) * 2 + core
    diagonal = (1 - chip) * 2 + (1 - core)

    def rows_of(chip_, core_):
        return pl.multiple_of(core_ * (2 * quarter) + chip_ * quarter, quarter)

    own = rows_of(chip, core)
    own_half = pl.multiple_of(core * (2 * quarter), 2 * quarter)
    sib_half = pl.multiple_of((1 - core) * (2 * quarter), 2 * quarter)

    def weight_copies(n):
        cols = cols_of(n)
        return (pltpu.make_async_copy(wo_hbm.at[:, cols], wo_v.at[:, cols], wsems.at[0, n]),
                pltpu.make_async_copy(wd_hbm.at[:, cols], wd_v.at[:, cols], wsems.at[1, n]))

    x_copy = pltpu.make_async_copy(x_hbm.at[pl.ds(own, quarter), :], x_v, sems.at[0])
    for n in range(pieces):
        for copy in weight_copies(n):
            copy.start()
    x_copy.start()

    barrier = pltpu.get_barrier_semaphore()
    for d in range(1, 4):
        pl.semaphore_signal(barrier, inc=1, device_id={'model': (me + d) % 4}, device_id_type=pl.DeviceIdType.MESH)
    pl.semaphore_wait(barrier, 3)

    kv_sends = []
    for d in range(1, 4):
        to = (me + d) % 4
        kv_sends.append(pltpu.make_async_remote_copy(
            src_ref=kv_v.at[pl.ds(pl.multiple_of(to * quarter, quarter), quarter), :], dst_ref=kv_all.at[me],
            send_sem=kv_send.at[d - 1], recv_sem=kv_recv.at[d - 1], device_id={'model': to}, device_id_type=pl.DeviceIdType.MESH))
    for copy in kv_sends:
        copy.start()
    kv_all[me] = kv_v[pl.ds(pl.multiple_of(me * quarter, quarter), quarter), :]

    def remote(src, dst, send, recv, n, to):
        return pltpu.make_async_remote_copy(src_ref=src, dst_ref=dst, send_sem=send.at[n], recv_sem=recv.at[n],
                                            device_id={'model': to}, device_id_type=pl.DeviceIdType.MESH)

    def rs(n):
        return remote(part.at[pl.ds(sib_half, 2 * quarter), cols_of(n)], from_sib.at[:, cols_of(n)], rs_send, rs_recv, n, sibling)

    def xs(n):
        return remote(half_sum.at[pl.ds(pl.multiple_of((1 - chip) * quarter, quarter), quarter), cols_of(n)], from_chip.at[:, cols_of(n)], xs_send, xs_recv, n, across)

    def y_piece(row, n):
        return y_v.at[pl.ds(row, quarter), cols_of(n)]

    def gx(n):
        return remote(y_piece(own, n), y_piece(own, n), gx_send, gx_recv, n, across)

    def gs(n):
        return remote(y_piece(own, n), y_piece(own, n), gs_send, gs_recv, n, sibling)

    def gf(n):
        if n == pieces - 1:
            return remote(y_piece(own, n), y_piece(own, n), gf_send, gf_recv, n, diagonal)
        other = rows_of(1 - chip, core)
        return remote(y_piece(other, n), y_piece(other, n), gf_send, gf_recv, n, sibling)

    def sum_chip(n):
        rs(n).wait_recv()
        half_sum[:, cols_of(n)] = part[pl.ds(own_half, 2 * quarter), cols_of(n)] + from_sib[:, cols_of(n)]
        xs(n).start()

    def finish(n):
        xs(n).wait_recv()
        cols = cols_of(n)
        mine = half_sum[pl.ds(pl.multiple_of(chip * quarter, quarter), quarter), cols] + from_chip[:, cols]
        y_v[pl.ds(own, quarter), cols] = (x_v[:, cols].astype(F32) + mine).astype(BF16)
        gx(n).start()
        if n == pieces - 1:
            gf(n).start()
        gs(n).start()

    def forward(n):
        gx(n).wait_recv()
        if n < pieces - 1:
            gf(n).start()

    for n in range(pieces):
        for copy in weight_copies(n):
            copy.wait()
        cols = cols_of(n)
        part[:, cols] = nn_dot(o_v[...], wo_v[:, cols]) + nn_dot(u_v[...], wd_v[:, cols])
        rs(n).start()
        if n >= 1:
            sum_chip(n - 1)
    sum_chip(pieces - 1)

    for copy in kv_sends:
        copy.wait_recv()
    for h in range(4):
        kv_rows[0, :, h, :] = kv_all[h, :, :head_dim].astype(F32)
        kv_rows[1, :, h, :] = kv_all[h, :, head_dim:].astype(F32)
    kn_ref[...] = kv_rows[0].astype(BF16)
    vn_ref[...] = kv_rows[1].astype(BF16)

    x_copy.wait()
    for n in range(pieces):
        finish(n)
    for n in range(pieces):
        forward(n)
    for n in range(pieces):
        gs(n).wait_recv()
        gf(n).wait_recv()

    for copy in kv_sends:
        copy.wait_send()
    for n in range(pieces):
        for copy in (rs(n), xs(n), gx(n), gs(n), gf(n)):
            copy.wait_send()


def write_kernel(y_v, kn_v, vn_v, y_hbm, kn_hbm, vn_hbm, sems):
    copies = [pltpu.make_async_copy(src, dst, sems.at[i]) for i, (src, dst) in enumerate([(y_v, y_hbm), (kn_v, kn_hbm), (vn_v, vn_hbm)])]
    for copy in copies:
        copy.start()
    for copy in copies:
        copy.wait()


def solution(mesh):
    def local_step(tokens, lengths, k_cache, v_cache, norm_gain, w_query, w_key, w_value, w_out, w_gate, w_up, w_down):
        batch, model_dim = tokens.shape
        kv_heads, context, head_dim = k_cache.shape[1:]
        ffn = w_gate.shape[1]
        q_width = w_query.shape[1]
        rows = 2 * batch
        max_tiles = batch * (context // CHUNK) + UNROLL
        any_spec = pl.BlockSpec(memory_space=pl.ANY)
        vmem_spec = pl.BlockSpec(memory_space=pltpu.VMEM)
        dma = pltpu.SemaphoreType.DMA

        pieces = ffn // COLS
        in_blocks = (batch, kv_heads, context // FIRST, FIRST, head_dim)
        hidden, attended, kv_new = pl.pallas_call(
            functools.partial(local_kernel, (batch, model_dim, head_dim, context)),
            name='attend_and_gate',
            out_shape=[pltpu.VMEM((batch, ffn), BF16), pltpu.VMEM((batch, q_width), BF16), pltpu.VMEM((batch, 2 * head_dim), BF16)],
            in_specs=[any_spec] * 10,
            out_specs=[vmem_spec] * 3,
            scratch_shapes=[
                pltpu.SMEM((1, batch), jnp.int32),
                pltpu.VMEM((1, batch), jnp.int32),
                pltpu.VMEM((batch, model_dim), BF16),
                pltpu.VMEM((model_dim,), BF16),
                pltpu.VMEM((model_dim, q_width), BF16),
                pltpu.VMEM((model_dim, head_dim), BF16),
                pltpu.VMEM((model_dim, head_dim), BF16),
                pltpu.VMEM((pieces, model_dim, COLS), BF16),
                pltpu.VMEM((pieces, model_dim, COLS), BF16),
                pltpu.VMEM((batch, FIRST, head_dim), BF16),
                pltpu.VMEM((batch, FIRST, head_dim), BF16),
                pltpu.VMEM((SLOTS, UNROLL * CHUNK // FIRST, FIRST, head_dim), BF16),
                pltpu.VMEM((SLOTS, UNROLL * CHUNK // FIRST, FIRST, head_dim), BF16),
                pltpu.VMEM((batch, model_dim), BF16),
                pltpu.SMEM((max_tiles,), jnp.int32),
                pltpu.SMEM((max_tiles // UNROLL + 1,), jnp.int32),
                pltpu.VMEM((rows, head_dim), BF16),
                pltpu.VMEM((rows, 128), F32),
                pltpu.VMEM((batch // GROUP, 2 * GROUP, GROUP * FIRST), F32),
                pltpu.VMEM((max_tiles, 2 * GROUP, CHUNK), F32),
                pltpu.VMEM((rows, 128), F32),
                pltpu.VMEM((batch, head_dim), F32),
                pltpu.VMEM((rows, 128), F32),
                pltpu.VMEM((rows, 128), F32),
                pltpu.VMEM((rows, head_dim), F32),
                dma((7,)),
                dma((2, pieces)),
                dma((2, 2)),
                dma((SLOTS,)),
                dma((SLOTS,)),
            ],
            compiler_params=pltpu.CompilerParams(has_side_effects=True, vmem_limit_bytes=54 << 20),
        )(lengths.reshape(1, batch), tokens, norm_gain, k_cache.reshape(in_blocks), v_cache.reshape(in_blocks), w_query, w_key, w_value, w_gate, w_up)

        quarter = batch // 4
        pieces = len(WIDTHS)
        new_shape = (quarter, kv_heads, head_dim)
        out_shapes = [(batch, model_dim), new_shape, new_shape]
        outs = pl.pallas_call(
            functools.partial(reduce_kernel, (batch, head_dim)),
            name='project_and_sum',
            out_shape=[pltpu.VMEM(shape, BF16) for shape in out_shapes],
            in_specs=[any_spec, vmem_spec, vmem_spec, vmem_spec, any_spec, any_spec],
            out_specs=[vmem_spec] * 3,
            scratch_shapes=[
                pltpu.VMEM((quarter, model_dim), BF16),
                pltpu.VMEM((4, quarter, 2 * head_dim), BF16),
                pltpu.VMEM((2, quarter, 4, head_dim), F32),
                pltpu.VMEM((q_width, model_dim), BF16),
                pltpu.VMEM((ffn, model_dim), BF16),
                pltpu.VMEM((batch, model_dim), F32),
                pltpu.VMEM((2 * quarter, model_dim), F32),
                pltpu.VMEM((2 * quarter, model_dim), F32),
                pltpu.VMEM((quarter, model_dim), F32),
                dma((1,)),
                dma((2, pieces)),
                dma((3,)), dma((3,)),
            ] + [dma((pieces,))] * 10,
            compiler_params=pltpu.CompilerParams(collective_id=0, has_side_effects=True, vmem_limit_bytes=48 << 20),
        )(tokens, hidden, attended, kv_new, w_out, w_down)
        return pl.pallas_call(
            write_kernel,
            name='write_results',
            out_shape=[jax.ShapeDtypeStruct(shape, BF16) for shape in out_shapes],
            in_specs=[vmem_spec] * 3,
            out_specs=[any_spec] * 3,
            scratch_shapes=[dma((3,))],
            compiler_params=pltpu.CompilerParams(has_side_effects=True, vmem_limit_bytes=4 << 20),
        )(*outs)

    in_specs = (P('replica', None), P('replica'), P('replica', None, None, None), P('replica', None, None, None), P(None), P(None, 'model'), P(None, None), P(None, None), P('model', None), P(None, 'model'), P(None, 'model'), P('model', None))
    out_specs = (P('replica', None), P(('replica', 'model'), None, None), P(('replica', 'model'), None, None))
    return jax.shard_map(local_step, mesh=mesh, in_specs=in_specs, out_specs=out_specs, check_vma=False)
```

```python
import functools
import math
import jax
import jax.numpy as jnp
from jax import lax
from jax.experimental import pallas as pl
from jax.experimental.pallas import tpu as pltpu
from jax.sharding import PartitionSpec as P

ROPE_BASE = 10000.0
NORM_EPS = 1e-6
MASK_VALUE = -1e30
F32 = jnp.float32
BF16 = jnp.bfloat16

FIRST = 32
GROUP = 8
CHUNK = 128
UNROLL = 16
SLOTS = 6
GATE_WIDTHS = (768, 768, 512, 256)
WIDTHS = (256, 256, 512, 512, 512, 256)


def iota(shape, dim):
    return lax.broadcasted_iota(jnp.int32, shape, dim)


def nt_dot(a, b):
    return lax.dot_general(a, b, (((1,), (1,)), ((), ())), preferred_element_type=F32)


def nn_dot(a, b):
    return jnp.dot(a, b, preferred_element_type=F32)


def interleave(first, second):
    pieces = []
    for r in range(0, first.shape[0], GROUP):
        pieces += [first[r:r + GROUP], second[r:r + GROUP]]
    return jnp.concatenate(pieces, axis=0)


def local_kernel(dims, len_hbm, x_hbm, gain_hbm, k_hbm, v_hbm, wq_hbm, wk_hbm, wv_hbm, wg_hbm, wu_hbm,
                 u_ref, o_ref, kv_ref,
                 len_s, len_v, x_v, gain_v, wq_v, wk_v, wv_v, wg_v, wu_v, kfirst, vfirst, kbuf, vbuf, h_v,
                 tile_s, size_s, q_rows, len_rows, s_first, s_buf, snew_v, vnew_v, m_v, l_v, acc_v,
                 sems, wsems, fsems, ksems, vsems):
    batch, model_dim, head_dim, context = dims
    half = head_dim // 2
    rows = 2 * GROUP
    groups = batch // GROUP
    me = lax.axis_index('model')
    n_pieces = len(GATE_WIDTHS)
    blocks = CHUNK // FIRST

    def gate_cols(n):
        return pl.ds(sum(GATE_WIDTHS[:n]), GATE_WIDTHS[n])

    def piece_copy(hbm, buf, n, which):
        return pltpu.make_async_copy(hbm.at[:, gate_cols(n)], buf.at[:, gate_cols(n)], wsems.at[which, n])

    def first_copy(hbm, buf, which, n):
        seqs = pl.ds(n * (batch // 2), batch // 2)
        return pltpu.make_async_copy(hbm.at[seqs, me, 0], buf.at[seqs], fsems.at[which, n])

    head_col = pl.multiple_of(me * head_dim, 128)
    small = [
        pltpu.make_async_copy(len_hbm, len_s, sems.at[0]),
        pltpu.make_async_copy(x_hbm, x_v, sems.at[1]),
        pltpu.make_async_copy(gain_hbm, gain_v, sems.at[2]),
        pltpu.make_async_copy(len_hbm, len_v, sems.at[6]),
        pltpu.make_async_copy(wq_hbm, wq_v, sems.at[3]),
        pltpu.make_async_copy(wk_hbm.at[:, pl.ds(head_col, head_dim)], wk_v, sems.at[4]),
        pltpu.make_async_copy(wv_hbm.at[:, pl.ds(head_col, head_dim)], wv_v, sems.at[5]),
    ]
    for copy in small:
        copy.start()
    for n in range(2):
        first_copy(k_hbm, kfirst, 0, n).start()
    for n in range(2):
        first_copy(v_hbm, vfirst, 1, n).start()
    for n in range(n_pieces):
        piece_copy(wg_hbm, wg_v, n, 0).start(priority=1)
        piece_copy(wu_hbm, wu_v, n, 1).start(priority=1)

    vbuf[...] = jnp.zeros_like(vbuf)
    small[0].wait()

    def fill(r, t):
        for i in range(GROUP):
            b = r * GROUP + i
            for c in range((context - FIRST + CHUNK - 1) // CHUNK):
                tile_s[t + c] = b * 8 + c
            t = t + lax.shift_right_logical(len_s[0, b] + (CHUNK - 1 - FIRST), CHUNK.bit_length() - 1)
        return t
    tiles = lax.fori_loop(0, groups, fill, 0)
    for j in range(UNROLL):
        tile_s[tiles + j] = 7
    bodies = (tiles + UNROLL - 1) // UNROLL

    def issue(hbm, buf, bsems, body):
        slot = lax.rem(body, SLOTS)
        total = 0
        for j in range(UNROLL):
            code = tile_s[body * UNROLL + j]
            b = lax.shift_right_logical(code, 3)
            start = jnp.minimum(1 + (code & 7) * blocks, context // FIRST - 1)
            end = lax.shift_right_logical(len_s[0, b] + (FIRST - 1), FIRST.bit_length() - 1)
            count = jnp.clip(end - start, 1, blocks)
            pltpu.make_async_copy(hbm.at[b, me, pl.ds(start, count)], buf.at[slot, pl.ds(j * blocks, count)], bsems.at[slot]).start()
            total += count
        size_s[body] = total

    def issue_both(body, _):
        issue(k_hbm, kbuf, ksems, body)
        issue(v_hbm, vbuf, vsems, body)
        return 0

    def wait_body(buf, bsems, body):
        slot = lax.rem(body, SLOTS)
        filled = buf.at[slot, pl.ds(0, size_s[body])]
        pltpu.make_async_copy(filled, filled, bsems.at[slot]).wait()

    lax.fori_loop(0, jnp.minimum(bodies, SLOTS), issue_both, 0)

    small[3].wait()
    ii, jj = iota((batch, batch), 0), iota((batch, batch), 1)
    len_col = jnp.sum(jnp.where(ii == jj, len_v[...].astype(F32), 0.0), axis=1, keepdims=True)
    len_wide = jnp.broadcast_to(len_col, (batch, 128))
    len_rows[...] = interleave(len_wide, len_wide)
    freq = jnp.exp(iota((1, half), 1).astype(F32) * (-2.0 * math.log(ROPE_BASE) / head_dim))
    angles = len_col * freq
    cos_part, sin_part = jnp.cos(angles), jnp.sin(angles)

    def rope(v):
        a, b = v[:, :half], v[:, half:]
        return jnp.concatenate([a * cos_part - b * sin_part, b * cos_part + a * sin_part], axis=1).astype(BF16)

    small[1].wait()
    small[2].wait()
    x = x_v[...].astype(F32)
    mean_sq = jnp.mean(x * x, axis=-1, keepdims=True)
    h_v[...] = (x * lax.rsqrt(mean_sq + NORM_EPS) * gain_v[...].astype(F32).reshape(1, model_dim)).astype(BF16)

    small[4].wait()
    h = h_v[...]
    q = nn_dot(h, wq_v[...])
    q_heads = [rope(q[:, n * head_dim:(n + 1) * head_dim]).astype(F32) for n in range(2)]
    q_rows[...] = interleave(*q_heads).astype(BF16)
    small[5].wait()
    small[6].wait()
    k_new = rope(nn_dot(h, wk_v[...]))
    v_new = nn_dot(h, wv_v[...]).astype(BF16)
    kv_ref[:, :head_dim] = k_new
    kv_ref[:, head_dim:] = v_new
    vnew_v[...] = v_new.astype(F32)
    scale = head_dim ** -0.5
    k_wide = k_new.astype(F32)
    s_new = [jnp.broadcast_to(jnp.sum(qh * k_wide, axis=1, keepdims=True) * scale, (batch, 128)) for qh in q_heads]
    snew_v[...] = interleave(*s_new)

    lane, sub = iota((rows, GROUP * FIRST), 1), iota((rows, GROUP * FIRST), 0)
    own_lane = lax.shift_right_logical(lane, FIRST.bit_length() - 1) == (sub & (GROUP - 1))
    token = (lane & (FIRST - 1)).astype(F32)
    for n in range(2):
        first_copy(k_hbm, kfirst, 0, n).wait()
    for g in range(groups):
        keys = kfirst[g * GROUP:(g + 1) * GROUP].reshape(GROUP * FIRST, head_dim)
        s = nt_dot(q_rows[g * rows:(g + 1) * rows, :], keys)
        reach = len_rows[g * rows:(g + 1) * rows, :]
        s = jnp.where(own_lane & (token < jnp.concatenate([reach, reach], axis=1)), s * scale, MASK_VALUE)
        s_first[g] = s
        m_v[g * rows:(g + 1) * rows, :] = jnp.maximum(snew_v[g * rows:(g + 1) * rows, :], jnp.maximum(s[:, :128], s[:, 128:]))

    lane, sub = iota((rows, CHUNK), 1), iota((rows, CHUNK), 0) & (GROUP - 1)

    def tile_of(t):
        code = tile_s[t]
        b = lax.shift_right_logical(code, 3)
        row = pl.multiple_of(lax.shift_right_logical(b, GROUP.bit_length() - 1) * rows, rows)
        return b & (GROUP - 1), row, FIRST + (code & 7) * CHUNK

    def score_body(body, _):
        wait_body(kbuf, ksems, body)
        slot = lax.rem(body, SLOTS)
        scores = []
        for j in range(UNROLL):
            i, row, begin = tile_of(body * UNROLL + j)
            s = nt_dot(q_rows[pl.ds(row, rows), :], kbuf[slot, j * blocks:(j + 1) * blocks].reshape(CHUNK, head_dim))
            valid = (sub == i) & ((lane + begin).astype(F32) < len_rows[pl.ds(row, rows), :])
            scores.append((row, jnp.where(valid, s * scale, MASK_VALUE)))
        for j, (row, s) in enumerate(scores):
            s_buf[body * UNROLL + j] = s
            m_v[pl.ds(row, rows), :] = jnp.maximum(m_v[pl.ds(row, rows), :], s)

        @pl.when(body + SLOTS < bodies)
        def _():
            issue(k_hbm, kbuf, ksems, body + SLOTS)
        return 0
    lax.fori_loop(0, bodies, score_body, 0)

    peak = jnp.max(m_v[...], axis=1, keepdims=True)
    m_v[...] = jnp.broadcast_to(peak, m_v.shape)

    for n in range(2):
        first_copy(v_hbm, vfirst, 1, n).wait()
    for g in range(groups):
        m = m_v[g * rows:(g + 1) * rows, :]
        p = jnp.exp(s_first[g] - jnp.concatenate([m, m], axis=1))
        l_v[g * rows:(g + 1) * rows, :] = p[:, :128] + p[:, 128:]
        acc_v[g * rows:(g + 1) * rows, :] = nn_dot(p.astype(BF16), vfirst[g * GROUP:(g + 1) * GROUP].reshape(GROUP * FIRST, head_dim))

    def value_body(body, _):
        wait_body(vbuf, vsems, body)
        slot = lax.rem(body, SLOTS)
        mixed = []
        for j in range(UNROLL):
            _, row, _ = tile_of(body * UNROLL + j)
            p = jnp.exp(s_buf[body * UNROLL + j] - m_v[pl.ds(row, rows), :])
            mixed.append((row, p, nn_dot(p.astype(BF16), vbuf[slot, j * blocks:(j + 1) * blocks].reshape(CHUNK, head_dim))))
        for row, p, o in mixed:
            l_v[pl.ds(row, rows), :] += p
            acc_v[pl.ds(row, rows), :] += o

        @pl.when(body + SLOTS < bodies)
        def _():
            issue(v_hbm, vbuf, vsems, body + SLOTS)
        return 0
    lax.fori_loop(0, bodies, value_body, 0)

    e_new = jnp.exp(snew_v[...] - m_v[...])
    total = jnp.sum(l_v[...], axis=1, keepdims=True) + e_new[:, :1]
    weight_new = e_new[:, :1].astype(BF16).astype(F32)
    mixed = (acc_v[...] + weight_new * interleave(vnew_v[...], vnew_v[...])) / total
    for head in range(2):
        o_head = jnp.concatenate([mixed[g * rows + head * GROUP:g * rows + (head + 1) * GROUP] for g in range(groups)], axis=0)
        o_ref[:, head * head_dim:(head + 1) * head_dim] = o_head.astype(BF16)

    for n in range(n_pieces):
        piece_copy(wg_hbm, wg_v, n, 0).wait()
        piece_copy(wu_hbm, wu_v, n, 1).wait()
        gate = nn_dot(h_v[...], wg_v[:, gate_cols(n)])
        up = nn_dot(h_v[...], wu_v[:, gate_cols(n)])
        u_ref[:, gate_cols(n)] = (gate * jax.nn.sigmoid(gate) * up).astype(BF16)


def reduce_kernel(dims, x_hbm, u_v, o_v, kv_v, wo_hbm, wd_hbm,
                  y_v, kn_ref, vn_ref,
                  x_v, kv_all, kv_rows, wo_v, wd_v, part, from_sib, half_sum, from_chip,
                  sems, wsems, kv_send, kv_recv, rs_send, rs_recv, xs_send, xs_recv, gx_send, gx_recv, gs_send, gs_recv, gf_send, gf_recv):
    batch, head_dim = dims
    quarter = batch // 4
    pieces = len(WIDTHS)

    def cols_of(n):
        return pl.ds(sum(WIDTHS[:n]), WIDTHS[n])

    me = lax.axis_index('model')
    chip, core = me // 2, me % 2
    sibling = chip * 2 + (1 - core)
    across = (1 - chip) * 2 + core
    diagonal = (1 - chip) * 2 + (1 - core)

    def rows_of(chip_, core_):
        return pl.multiple_of(core_ * (2 * quarter) + chip_ * quarter, quarter)

    own = rows_of(chip, core)
    own_half = pl.multiple_of(core * (2 * quarter), 2 * quarter)
    sib_half = pl.multiple_of((1 - core) * (2 * quarter), 2 * quarter)

    def weight_copies(n):
        cols = cols_of(n)
        return (pltpu.make_async_copy(wo_hbm.at[:, cols], wo_v.at[:, cols], wsems.at[0, n]),
                pltpu.make_async_copy(wd_hbm.at[:, cols], wd_v.at[:, cols], wsems.at[1, n]))

    x_copy = pltpu.make_async_copy(x_hbm.at[pl.ds(own, quarter), :], x_v, sems.at[0])
    for n in range(pieces):
        for copy in weight_copies(n):
            copy.start()
    x_copy.start()

    barrier = pltpu.get_barrier_semaphore()
    for d in range(1, 4):
        pl.semaphore_signal(barrier, inc=1, device_id={'model': (me + d) % 4}, device_id_type=pl.DeviceIdType.MESH)
    pl.semaphore_wait(barrier, 3)

    kv_sends = []
    for d in range(1, 4):
        to = (me + d) % 4
        kv_sends.append(pltpu.make_async_remote_copy(
            src_ref=kv_v.at[pl.ds(pl.multiple_of(to * quarter, quarter), quarter), :], dst_ref=kv_all.at[me],
            send_sem=kv_send.at[d - 1], recv_sem=kv_recv.at[d - 1], device_id={'model': to}, device_id_type=pl.DeviceIdType.MESH))
    for copy in kv_sends:
        copy.start()
    kv_all[me] = kv_v[pl.ds(pl.multiple_of(me * quarter, quarter), quarter), :]

    def remote(src, dst, send, recv, n, to):
        return pltpu.make_async_remote_copy(src_ref=src, dst_ref=dst, send_sem=send.at[n], recv_sem=recv.at[n],
                                            device_id={'model': to}, device_id_type=pl.DeviceIdType.MESH)

    def rs(n):
        return remote(part.at[pl.ds(sib_half, 2 * quarter), cols_of(n)], from_sib.at[:, cols_of(n)], rs_send, rs_recv, n, sibling)

    def xs(n):
        return remote(half_sum.at[pl.ds(pl.multiple_of((1 - chip) * quarter, quarter), quarter), cols_of(n)], from_chip.at[:, cols_of(n)], xs_send, xs_recv, n, across)

    def y_piece(row, n):
        return y_v.at[pl.ds(row, quarter), cols_of(n)]

    def gx(n):
        return remote(y_piece(own, n), y_piece(own, n), gx_send, gx_recv, n, across)

    def gs(n):
        return remote(y_piece(own, n), y_piece(own, n), gs_send, gs_recv, n, sibling)

    def gf(n):
        if n == pieces - 1:
            return remote(y_piece(own, n), y_piece(own, n), gf_send, gf_recv, n, diagonal)
        other = rows_of(1 - chip, core)
        return remote(y_piece(other, n), y_piece(other, n), gf_send, gf_recv, n, sibling)

    def sum_chip(n):
        rs(n).wait_recv()
        half_sum[:, cols_of(n)] = part[pl.ds(own_half, 2 * quarter), cols_of(n)] + from_sib[:, cols_of(n)]
        xs(n).start()

    def finish(n):
        xs(n).wait_recv()
        cols = cols_of(n)
        mine = half_sum[pl.ds(pl.multiple_of(chip * quarter, quarter), quarter), cols] + from_chip[:, cols]
        y_v[pl.ds(own, quarter), cols] = (x_v[:, cols].astype(F32) + mine).astype(BF16)
        gx(n).start()
        if n == pieces - 1:
            gf(n).start()
        gs(n).start()

    def forward(n):
        gx(n).wait_recv()
        if n < pieces - 1:
            gf(n).start()

    for n in range(pieces):
        for copy in weight_copies(n):
            copy.wait()
        cols = cols_of(n)
        part[:, cols] = nn_dot(o_v[...], wo_v[:, cols]) + nn_dot(u_v[...], wd_v[:, cols])
        rs(n).start()
        if n >= 1:
            sum_chip(n - 1)
    sum_chip(pieces - 1)

    for copy in kv_sends:
        copy.wait_recv()
    for h in range(4):
        kv_rows[0, :, h, :] = kv_all[h, :, :head_dim].astype(F32)
        kv_rows[1, :, h, :] = kv_all[h, :, head_dim:].astype(F32)
    kn_ref[...] = kv_rows[0].astype(BF16)
    vn_ref[...] = kv_rows[1].astype(BF16)

    x_copy.wait()
    for n in range(pieces):
        finish(n)
    for n in range(pieces):
        forward(n)
    for n in range(pieces):
        gs(n).wait_recv()
        gf(n).wait_recv()

    for copy in kv_sends:
        copy.wait_send()
    for n in range(pieces):
        for copy in (rs(n), xs(n), gx(n), gs(n), gf(n)):
            copy.wait_send()


def write_kernel(y_v, kn_v, vn_v, y_hbm, kn_hbm, vn_hbm, sems):
    copies = [pltpu.make_async_copy(src, dst, sems.at[i]) for i, (src, dst) in enumerate([(y_v, y_hbm), (kn_v, kn_hbm), (vn_v, vn_hbm)])]
    for copy in copies:
        copy.start()
    for copy in copies:
        copy.wait()


def solution(mesh):
    def local_step(tokens, lengths, k_cache, v_cache, norm_gain, w_query, w_key, w_value, w_out, w_gate, w_up, w_down):
        batch, model_dim = tokens.shape
        kv_heads, context, head_dim = k_cache.shape[1:]
        ffn = w_gate.shape[1]
        q_width = w_query.shape[1]
        rows = 2 * batch
        max_tiles = batch * (context // CHUNK) + UNROLL
        any_spec = pl.BlockSpec(memory_space=pl.ANY)
        vmem_spec = pl.BlockSpec(memory_space=pltpu.VMEM)
        dma = pltpu.SemaphoreType.DMA

        pieces = len(GATE_WIDTHS)
        in_blocks = (batch, kv_heads, context // FIRST, FIRST, head_dim)
        hidden, attended, kv_new = pl.pallas_call(
            functools.partial(local_kernel, (batch, model_dim, head_dim, context)),
            name='attend_and_gate',
            out_shape=[pltpu.VMEM((batch, ffn), BF16), pltpu.VMEM((batch, q_width), BF16), pltpu.VMEM((batch, 2 * head_dim), BF16)],
            in_specs=[any_spec] * 10,
            out_specs=[vmem_spec] * 3,
            scratch_shapes=[
                pltpu.SMEM((1, batch), jnp.int32),
                pltpu.VMEM((1, batch), jnp.int32),
                pltpu.VMEM((batch, model_dim), BF16),
                pltpu.VMEM((model_dim,), BF16),
                pltpu.VMEM((model_dim, q_width), BF16),
                pltpu.VMEM((model_dim, head_dim), BF16),
                pltpu.VMEM((model_dim, head_dim), BF16),
                pltpu.VMEM((model_dim, ffn), BF16),
                pltpu.VMEM((model_dim, ffn), BF16),
                pltpu.VMEM((batch, FIRST, head_dim), BF16),
                pltpu.VMEM((batch, FIRST, head_dim), BF16),
                pltpu.VMEM((SLOTS, UNROLL * CHUNK // FIRST, FIRST, head_dim), BF16),
                pltpu.VMEM((SLOTS, UNROLL * CHUNK // FIRST, FIRST, head_dim), BF16),
                pltpu.VMEM((batch, model_dim), BF16),
                pltpu.SMEM((max_tiles,), jnp.int32),
                pltpu.SMEM((max_tiles // UNROLL + 1,), jnp.int32),
                pltpu.VMEM((rows, head_dim), BF16),
                pltpu.VMEM((rows, 128), F32),
                pltpu.VMEM((batch // GROUP, 2 * GROUP, GROUP * FIRST), F32),
                pltpu.VMEM((max_tiles, 2 * GROUP, CHUNK), F32),
                pltpu.VMEM((rows, 128), F32),
                pltpu.VMEM((batch, head_dim), F32),
                pltpu.VMEM((rows, 128), F32),
                pltpu.VMEM((rows, 128), F32),
                pltpu.VMEM((rows, head_dim), F32),
                dma((7,)),
                dma((2, pieces)),
                dma((2, 2)),
                dma((SLOTS,)),
                dma((SLOTS,)),
            ],
            compiler_params=pltpu.CompilerParams(has_side_effects=True, vmem_limit_bytes=54 << 20),
        )(lengths.reshape(1, batch), tokens, norm_gain, k_cache.reshape(in_blocks), v_cache.reshape(in_blocks), w_query, w_key, w_value, w_gate, w_up)

        quarter = batch // 4
        pieces = len(WIDTHS)
        new_shape = (quarter, kv_heads, head_dim)
        out_shapes = [(batch, model_dim), new_shape, new_shape]
        outs = pl.pallas_call(
            functools.partial(reduce_kernel, (batch, head_dim)),
            name='project_and_sum',
            out_shape=[pltpu.VMEM(shape, BF16) for shape in out_shapes],
            in_specs=[any_spec, vmem_spec, vmem_spec, vmem_spec, any_spec, any_spec],
            out_specs=[vmem_spec] * 3,
            scratch_shapes=[
                pltpu.VMEM((quarter, model_dim), BF16),
                pltpu.VMEM((4, quarter, 2 * head_dim), BF16),
                pltpu.VMEM((2, quarter, 4, head_dim), F32),
                pltpu.VMEM((q_width, model_dim), BF16),
                pltpu.VMEM((ffn, model_dim), BF16),
                pltpu.VMEM((batch, model_dim), F32),
                pltpu.VMEM((2 * quarter, model_dim), F32),
                pltpu.VMEM((2 * quarter, model_dim), F32),
                pltpu.VMEM((quarter, model_dim), F32),
                dma((1,)),
                dma((2, pieces)),
                dma((3,)), dma((3,)),
            ] + [dma((pieces,))] * 10,
            compiler_params=pltpu.CompilerParams(collective_id=0, has_side_effects=True, vmem_limit_bytes=48 << 20),
        )(tokens, hidden, attended, kv_new, w_out, w_down)
        return pl.pallas_call(
            write_kernel,
            name='write_results',
            out_shape=[jax.ShapeDtypeStruct(shape, BF16) for shape in out_shapes],
            in_specs=[vmem_spec] * 3,
            out_specs=[any_spec] * 3,
            scratch_shapes=[dma((3,))],
            compiler_params=pltpu.CompilerParams(has_side_effects=True, vmem_limit_bytes=4 << 20),
        )(*outs)

    in_specs = (P('replica', None), P('replica'), P('replica', None, None, None), P('replica', None, None, None), P(None), P(None, 'model'), P(None, None), P(None, None), P('model', None), P(None, 'model'), P(None, 'model'), P('model', None))
    out_specs = (P('replica', None), P(('replica', 'model'), None, None), P(('replica', 'model'), None, None))
    return jax.shard_map(local_step, mesh=mesh, in_specs=in_specs, out_specs=out_specs, check_vma=False)
```
